16 devices in a mesh: model: 4 (over z, y), fsdp: 4 (over x, core).
Axes of the slice: x: 2, y: 2, z: 2, core: 2. Of those that a mesh axis runs over, the one named last changes fastest.
Arguments:
- tok_ids: int32 [4, 2048], P('fsdp')
- tok_labels: int32 [4, 2048], P('fsdp')
- emb_table: bfloat16 [50304, 768], P(('model', 'fsdp'))
- w_gate: bfloat16 [768, 3072], P('fsdp')
- w_up: bfloat16 [768, 3072], P('fsdp')
- w_down: bfloat16 [3072, 768], P('fsdp')
- gain_in: float32 [768], replicated
- gain_out: float32 [768], replicated
Outputs:
- output 1: float32 [], replicated
- output 2: float32 [50304, 768], P(('model', 'fsdp'))
- output 3: float32 [768, 3072], P('fsdp')
- output 4: float32 [768, 3072], P('fsdp')
- output 5: float32 [3072, 768], P('fsdp')
All inputs are finite; a program needn't handle non-finite values.
Results may differ from the reference program's by a relative error of at most 0.0100315.
Values are sent between devices in bfloat16 or wider.
A program may use at most 1 GiB of HBM per device.

```python
import jax
import jax.numpy as jnp
from jax import lax

V = 50304
D = 768
F = 3072
BATCH = 4
SEQ = 2048
HEAD_BLOCK = 64
EPS = 1e-6


def draw_tokens(base_key):
    id_key, label_key = jax.random.split(base_key)
    tok_ids = jax.random.randint(id_key, (BATCH, SEQ), 0, V, dtype=jnp.int32)
    tok_ids = tok_ids.at[0, 0].set(0).at[BATCH - 1, SEQ - 1].set(V - 1)
    tok_labels = jax.random.randint(label_key, (BATCH, SEQ), 0, V, dtype=jnp.int32)
    tok_labels = tok_labels.at[0, 0].set(V - 1).at[BATCH - 1, SEQ - 1].set(0)
    return tok_ids, tok_labels


def setup_inputs(seed: int = 0) -> dict:
    rng_keys = jax.random.split(jax.random.key(seed), 7)
    tok_ids, tok_labels = draw_tokens(rng_keys[0])
    emb_table = (jax.random.normal(rng_keys[1], (V, D), jnp.float32) * D ** -0.5).astype(jnp.bfloat16)
    w_gate = (jax.random.normal(rng_keys[2], (D, F), jnp.float32) * D ** -0.5).astype(jnp.bfloat16)
    w_up = (jax.random.normal(rng_keys[3], (D, F), jnp.float32) * D ** -0.5).astype(jnp.bfloat16)
    w_down = (jax.random.normal(rng_keys[4], (F, D), jnp.float32) * (2.0 * (F * D) ** -0.5)).astype(jnp.bfloat16)
    gain_in = jax.random.uniform(rng_keys[5], (D,), jnp.float32, 0.5, 1.5)
    gain_out = jax.random.uniform(rng_keys[6], (D,), jnp.float32, 0.5, 1.5)
    return {"tok_ids": tok_ids, "tok_labels": tok_labels, "emb_table": emb_table, "w_gate": w_gate, "w_up": w_up, "w_down": w_down, "gain_in": gain_in, "gain_out": gain_out}


def rms_scale(values, gain_vec):
    mean_sq = jnp.mean(values * values, axis=-1, keepdims=True)
    return values * lax.rsqrt(mean_sq + EPS) * gain_vec


def reference(tok_ids, tok_labels, emb_table, w_gate, w_up, w_down, gain_in, gain_out):
    num_tokens = BATCH * SEQ
    flat_ids = tok_ids.reshape(num_tokens)
    flat_labels = tok_labels.reshape(num_tokens)
    x_emb = emb_table[flat_ids].astype(jnp.float32)
    normed_in, norm_in_back = jax.vjp(lambda values: rms_scale(values, gain_in), x_emb)
    normed_bf = normed_in.astype(jnp.bfloat16)
    gate_f = jnp.dot(normed_bf, w_gate, preferred_element_type=jnp.float32).astype(jnp.bfloat16).astype(jnp.float32)
    up_f = jnp.dot(normed_bf, w_up, preferred_element_type=jnp.float32).astype(jnp.bfloat16).astype(jnp.float32)
    gate_sig = jax.nn.sigmoid(gate_f)
    silu_gate = gate_f * gate_sig
    act_bf = (silu_gate * up_f).astype(jnp.bfloat16)
    mlp_out = jnp.dot(act_bf, w_down, preferred_element_type=jnp.float32).astype(jnp.bfloat16)
    h_res = x_emb + mlp_out.astype(jnp.float32)
    hn_f, norm_out_back = jax.vjp(lambda values: rms_scale(values, gain_out), h_res)
    hn_bf = hn_f.astype(jnp.bfloat16)
    num_blocks = num_tokens // HEAD_BLOCK
    hn_blocks = hn_bf.reshape(num_blocks, HEAD_BLOCK, D)
    label_blocks = flat_labels.reshape(num_blocks, HEAD_BLOCK)

    def head_step(d_head, block_in):
        hn_blk, label_blk = block_in
        logits = jnp.dot(hn_blk, emb_table.T, preferred_element_type=jnp.float32)
        row_max = jnp.max(logits, axis=-1, keepdims=True)
        exp_shift = jnp.exp(logits - row_max)
        sum_exp = jnp.sum(exp_shift, axis=-1, keepdims=True)
        onehot = lax.broadcasted_iota(jnp.int32, logits.shape, 1) == label_blk[:, None]
        label_logit = jnp.sum(jnp.where(onehot, logits, 0.0), axis=-1)
        tok_loss = row_max[:, 0] + jnp.log(sum_exp[:, 0]) - label_logit
        soft_probs = exp_shift / sum_exp
        d_logits = (jnp.where(onehot, soft_probs - 1.0, soft_probs) / num_tokens).astype(jnp.bfloat16)
        d_head = d_head + jnp.dot(d_logits.T, hn_blk, preferred_element_type=jnp.float32)
        d_hn = jnp.dot(d_logits, emb_table, preferred_element_type=jnp.float32)
        return d_head, (tok_loss, d_hn)

    d_head, (tok_losses, d_hn_blocks) = lax.scan(head_step, jnp.zeros((V, D), jnp.float32), (hn_blocks, label_blocks))
    loss = jnp.sum(tok_losses) / num_tokens
    d_hn = d_hn_blocks.reshape(num_tokens, D)
    d_hidden = norm_out_back(d_hn)[0]
    d_mlp = d_hidden.astype(jnp.bfloat16)
    d_act = jnp.dot(d_mlp, w_down.T, preferred_element_type=jnp.float32)
    grad_down = jnp.dot(act_bf.T, d_mlp, preferred_element_type=jnp.float32)
    d_gate = (d_act * up_f * (gate_sig * (1.0 + gate_f * (1.0 - gate_sig)))).astype(jnp.bfloat16)
    d_up = (d_act * silu_gate).astype(jnp.bfloat16)
    grad_gate = jnp.dot(normed_bf.T, d_gate, preferred_element_type=jnp.float32)
    grad_up = jnp.dot(normed_bf.T, d_up, preferred_element_type=jnp.float32)
    d_normed = jnp.dot(d_gate, w_gate.T, preferred_element_type=jnp.float32) + jnp.dot(d_up, w_up.T, preferred_element_type=jnp.float32)
    d_x = d_hidden + norm_in_back(d_normed)[0]
    d_in = jax.ops.segment_sum(d_x, flat_ids, num_segments=V)
    grad_table = d_head + d_in
    return (loss, grad_table, grad_gate, grad_up, grad_down)
```

```python
import functools

import jax
import jax.numpy as jnp
from jax import lax
from jax.experimental import pallas as pl
from jax.experimental.pallas import tpu as pltpu
from jax.sharding import PartitionSpec as P

EPS = 1e-6
MESH = pl.DeviceIdType.MESH
AXES = ("model", "fsdp")
BF = jnp.bfloat16
F32 = jnp.float32
ROUND_ROWS = 64
VMEM_LIMIT = 64 * 1024 * 1024 - 128 * 1024


def rms_scale(values, gain_vec):
    mean_sq = jnp.mean(values * values, axis=-1, keepdims=True)
    return values * lax.rsqrt(mean_sq + EPS) * gain_vec


def my_place():
    m = lax.axis_index("model")
    f = lax.axis_index("fsdp")
    return (f // 2, m % 2, m // 2, f % 2)


def flipped(place, bits, core=False):
    x, y, z, c = place
    if bits & 1:
        x = 1 - x
    if bits & 2:
        y = 1 - y
    if bits & 4:
        z = 1 - z
    if core:
        c = 1 - c
    return (x, y, z, c)


def mesh_id(place):
    x, y, z, c = place
    return (2 * z + y, 2 * x + c)


def greet(place, bit_list, core):
    barrier = pltpu.get_barrier_semaphore()
    peers = [flipped(place, b) for b in bit_list] + ([flipped(place, 0, True)] if core else [])
    for peer in peers:
        pl.semaphore_signal(barrier, inc=1, device_id=mesh_id(peer), device_id_type=MESH)
    pl.semaphore_wait(barrier, len(peers))


ORDERS = ((1, 2, 4), (2, 4, 1), (4, 1, 2))


def subsets(bits):
    out = [0]
    for b in bits:
        out = out + [o | b for o in out]
    return out


def gather_kernel(parts, rows, in_ref, out_ref, local_sem, send_sem, recv_sem, core_send, core_recv):
    me = my_place()
    greet(me, (1, 2, 4), True)

    def block_of(place):
        m, f = mesh_id(place)
        return (m * 4 + f) * rows

    def out_part(place, color):
        lo, count = parts[color]
        return out_ref.at[pl.ds(pl.multiple_of(block_of(place) + lo, 8), count)]

    local = pltpu.make_async_copy(in_ref, out_ref.at[pl.ds(pl.multiple_of(block_of(me), 8), rows)], local_sem)
    local.start()
    sends = []

    def slot(color, stage, index):
        return color * 8 + (1 << stage) + index

    def chip_send(color, stage, index, bits):
        lo, count = parts[color]
        src = in_ref.at[pl.ds(lo, count)] if bits == 0 else out_part(flipped(me, bits), color)
        k = slot(color, stage, index)
        cp = pltpu.make_async_remote_copy(
            src_ref=src, dst_ref=out_part(flipped(me, bits), color),
            send_sem=send_sem.at[k], recv_sem=recv_sem.at[k],
            device_id=mesh_id(flipped(me, ORDERS[color][stage])), device_id_type=MESH)
        cp.start()
        sends.append(cp)

    def core_copy(color, bits, k):
        lo, count = parts[color]
        src = in_ref.at[pl.ds(lo, count)] if bits == 0 else out_part(flipped(me, bits), color)
        cp = pltpu.make_async_remote_copy(
            src_ref=src, dst_ref=out_part(flipped(me, bits), color),
            send_sem=core_send.at[k], recv_sem=core_recv.at[k],
            device_id=mesh_id(flipped(me, 0, True)), device_id_type=MESH)
        cp.start()
        sends.append(cp)

    for stage in range(3):
        for color in range(3):
            chip_send(color, stage, 0, 0)
    for color in range(3):
        core_copy(color, 0, color * 8)
    for stage in range(3):
        for index in range(1 << stage):
            for color in range(3):
                order = ORDERS[color]
                held = subsets(order[:stage])[index]
                bits = held | order[stage]
                k = slot(color, stage, index)
                pltpu.make_async_remote_copy(
                    src_ref=out_part(flipped(me, bits), color), dst_ref=out_part(flipped(me, bits), color),
                    send_sem=send_sem.at[k], recv_sem=recv_sem.at[k],
                    device_id=mesh_id(flipped(me, order[stage])), device_id_type=MESH).wait_recv()
                for later in range(stage + 1, 3):
                    chip_send(color, later, subsets(order[:later]).index(bits), bits)
                core_copy(color, bits, k)
    for color in range(3):
        for bits in range(8):
            order = ORDERS[color]
            if bits == 0:
                k = color * 8
            else:
                stage = max(s for s in range(3) if bits & order[s])
                k = slot(color, stage, subsets(order[:stage]).index(bits & ~order[stage]))
            dst = out_part(flipped(me, bits, True), color)
            pltpu.make_async_remote_copy(
                src_ref=dst, dst_ref=dst, send_sem=core_send.at[k], recv_sem=core_recv.at[k],
                device_id=mesh_id(flipped(me, 0, True)), device_id_type=MESH).wait_recv()
    for cp in sends:
        cp.wait_send()
    local.wait()


def gather_all(values, parts, collective_id):
    rows, width = values.shape
    any_spec = pl.BlockSpec(memory_space=pl.ANY)
    return pl.pallas_call(
        functools.partial(gather_kernel, parts, rows),
        out_shape=jax.ShapeDtypeStruct((16 * rows, width), values.dtype),
        in_specs=[any_spec], out_specs=any_spec,
        scratch_shapes=[pltpu.SemaphoreType.DMA, pltpu.SemaphoreType.DMA((24,)), pltpu.SemaphoreType.DMA((24,)),
                        pltpu.SemaphoreType.DMA((24,)), pltpu.SemaphoreType.DMA((24,))],
        compiler_params=pltpu.CompilerParams(collective_id=collective_id, has_side_effects=True),
        name=f"gather_all_{collective_id}",
    )(values)


CHUNK = 8


def add_rows(dst, slot_a, src, slot_b, rows):
    def body(i, carry):
        at = pl.ds(pl.multiple_of(i * CHUNK, CHUNK), CHUNK)
        dst[slot_a, at, :] = dst[slot_a, at, :] + src[slot_b, at, :]
        return carry

    lax.fori_loop(0, rows // CHUNK, body, 0)


BLOCK_ORDER = (7, 6, 5, 3, 4, 2, 1, 0)


def reduce_kernel(views, spread, *refs):
    n_in = max(v[0] for v in views) + 1
    ins = refs[:n_in]
    outs = refs[n_in:n_in + 3]
    accs = refs[n_in + 3:n_in + 6]
    pairs = refs[n_in + 6:n_in + 9]
    boxes = refs[n_in + 9:n_in + 12]
    load_sem, core_send, core_recv, send_sem, recv_sem, out_sem, sp_send, sp_recv = refs[n_in + 12:]
    me = my_place()
    greet(me, (1, 2, 4), True)
    sends = []
    loads = {}

    def source(color, place):
        which, rows, start = views[color]
        m, f = mesh_id(place)
        return ins[which].at[pl.ds(pl.multiple_of(start(m, f), 8), rows)]

    def core_copy(color, bits):
        k = color * 8 + bits
        return pltpu.make_async_remote_copy(
            src_ref=source(color, flipped(me, bits, True)), dst_ref=pairs[color].at[bits],
            send_sem=core_send.at[k], recv_sem=core_recv.at[k],
            device_id=mesh_id(flipped(me, 0, True)), device_id_type=MESH)

    for bits in BLOCK_ORDER:
        for color in range(3):
            cp = core_copy(color, bits)
            cp.start()
            sends.append(cp)
            ld = pltpu.make_async_copy(source(color, flipped(me, bits)), accs[color].at[bits], load_sem.at[color * 8 + bits])
            ld.start()
            loads[color, bits] = ld

    def stage_of(color, bits):
        order = ORDERS[color]
        for s in range(3):
            if bits & order[s]:
                return s
        return 3

    def box_slot(color, stage, bits):
        order = ORDERS[color]
        rest = subsets(order[stage + 1:])
        return (0, 4, 6)[stage] + rest.index(bits)

    def chip_copy(color, stage, bits):
        order = ORDERS[color]
        slot = box_slot(color, stage, bits & ~order[stage])
        k = color * 8 + slot
        return pltpu.make_async_remote_copy(
            src_ref=accs[color].at[bits], dst_ref=boxes[color].at[slot],
            send_sem=send_sem.at[k], recv_sem=recv_sem.at[k],
            device_id=mesh_id(flipped(me, order[stage])), device_id_type=MESH)

    for bits in BLOCK_ORDER:
        for color in range(3):
            loads[color, bits].wait()
            core_copy(color, bits).wait_recv()
            add_rows(accs[color], bits, pairs[color], bits, views[color][1])
            if stage_of(color, bits) == 0:
                cp = chip_copy(color, 0, bits)
                cp.start()
                sends.append(cp)
    for stage in range(3):
        for color in range(3):
            order = ORDERS[color]
            arriving = subsets(order[stage + 1:])
            for bits in sorted(arriving, key=lambda b: stage_of(color, b)):
                slot = box_slot(color, stage, bits)
                chip_copy(color, stage, bits | order[stage]).wait_recv()
                add_rows(accs[color], bits, boxes[color], slot, views[color][1])
                if stage_of(color, bits) == stage + 1 and stage < 2:
                    cp = chip_copy(color, stage + 1, bits)
                    cp.start()
                    sends.append(cp)
    locals_ = []
    if spread is None:
        for color in range(3):
            cp = pltpu.make_async_copy(accs[color].at[0], outs[color], out_sem.at[color])
            cp.start()
            locals_.append(cp)
    else:
        halves = ((2, 4), (4, 2))

        def target(color, place, half):
            rows = views[color][1]
            m, f = mesh_id(place)
            return outs[color].at[pl.ds(pl.multiple_of(m * rows + half * (rows // 2), 8), rows // 2)]

        def spread_copy(color, half, step, bits):
            rows = views[color][1]
            first, second = halves[half]
            src = accs[color].at[0, pl.ds(half * (rows // 2), rows // 2)] if bits == 0 else target(color, flipped(me, bits), half)
            k = (color * 2 + half) * 3 + step
            return pltpu.make_async_remote_copy(
                src_ref=src, dst_ref=target(color, flipped(me, bits), half),
                send_sem=sp_send.at[k], recv_sem=sp_recv.at[k],
                device_id=mesh_id(flipped(me, first if step == 0 else second)), device_id_type=MESH)

        for color in range(3):
            rows = views[color][1]
            m, f = mesh_id(me)
            cp = pltpu.make_async_copy(accs[color].at[0], outs[color].at[pl.ds(pl.multiple_of(m * rows, 8), rows)], out_sem.at[color])
            cp.start()
            locals_.append(cp)
            for half in range(2):
                for step in range(2):
                    cp = spread_copy(color, half, step, 0)
                    cp.start()
                    sends.append(cp)
        for color in range(3):
            for half in range(2):
                first, second = halves[half]
                spread_arrival(spread_copy, target, me, color, half, 0, first)
                cp = spread_copy(color, half, 2, first)
                cp.start()
                sends.append(cp)
        for color in range(3):
            for half in range(2):
                first, second = halves[half]
                spread_arrival(spread_copy, target, me, color, half, 1, second)
                spread_arrival(spread_copy, target, me, color, half, 2, first | second)
    for cp in sends:
        cp.wait_send()
    for cp in locals_:
        cp.wait()


def spread_arrival(spread_copy, target, me, color, half, step, bits):
    spread_copy(color, half, step, bits).wait_recv()


def reduce_all(arrays, views, out_shapes, piece_shapes, spread, collective_id):
    any_spec = pl.BlockSpec(memory_space=pl.ANY)
    scratch = []
    for count in (8, 8, 7):
        for shape in piece_shapes:
            scratch.append(pltpu.VMEM((count,) + shape, F32))
    sems = [pltpu.SemaphoreType.DMA((24,))] * 5 + [pltpu.SemaphoreType.DMA((3,))] + [pltpu.SemaphoreType.DMA((18,))] * 2
    return pl.pallas_call(
        functools.partial(reduce_kernel, views, spread),
        out_shape=[jax.ShapeDtypeStruct(s, F32) for s in out_shapes],
        in_specs=[any_spec] * len(arrays), out_specs=[any_spec] * 3,
        scratch_shapes=scratch + sems,
        compiler_params=pltpu.CompilerParams(collective_id=collective_id, has_side_effects=True, vmem_limit_bytes=VMEM_LIMIT),
        name=f"reduce_all_{collective_id}",
    )(*arrays)


def logits_kernel(chunks, vocab, hn_ref, emb_ref, lab_ref, z_ref, st_ref):
    hn = hn_ref[...]
    lab = lab_ref[...]
    top = None
    lab_z = None
    for lo, count in chunks:
        z = lax.dot_general(hn, emb_ref[lo:lo + count, :], (((1,), (1,)), ((), ())), preferred_element_type=F32)
        z_ref[:, lo:lo + count] = z
        col = lax.broadcasted_iota(jnp.int32, z.shape, 1) + lo
        picked = jnp.sum(jnp.where(col == lab, z, 0.0), axis=1, keepdims=True)
        if lo + count > vocab:
            z = jnp.where(col < vocab, z, -jnp.inf)
        peak = jnp.max(z, axis=1, keepdims=True)
        top = peak if top is None else jnp.maximum(top, peak)
        lab_z = picked if lab_z is None else lab_z + picked
    total = None
    for lo, count in chunks:
        z = z_ref[:, lo:lo + count]
        e = jnp.exp(z - top)
        if lo + count > vocab:
            col = lax.broadcasted_iota(jnp.int32, z.shape, 1) + lo
            e = jnp.where(col < vocab, e, 0.0)
        part = jnp.sum(e, axis=1, keepdims=True)
        total = part if total is None else total + part
    lane = lax.broadcasted_iota(jnp.int32, st_ref.shape, 1)
    st_ref[...] = jnp.where(lane == 0, top, jnp.where(lane == 1, total, lab_z))


def grads_kernel(chunks, vocab, inv_n, z_ref, hn_ref, emb_ref, st_ref, lab_ref, dhn_ref, de_ref):
    @pl.when(pl.program_id(0) == 0)
    def _():
        de_ref[...] = jnp.zeros_like(de_ref)

    hn = hn_ref[...]
    lab = lab_ref[...]
    top = st_ref[:, 0:1]
    inv_sum = 1.0 / st_ref[:, 1:2]
    acc = None
    for lo, count in chunks:
        z = z_ref[:, lo:lo + count]
        p = jnp.exp(z - top) * inv_sum
        col = lax.broadcasted_iota(jnp.int32, z.shape, 1) + lo
        p = jnp.where(col == lab, p - 1.0, p) * inv_n
        if lo + count > vocab:
            p = jnp.where(col < vocab, p, 0.0)
        dz = p.astype(BF)
        part = jnp.dot(dz, emb_ref[lo:lo + count, :], preferred_element_type=F32)
        acc = part if acc is None else acc + part
        de_ref[lo:lo + count, :] += lax.dot_general(dz, hn, (((0,), (0,)), ((), ())), preferred_element_type=F32)
    dhn_ref[...] = acc


def make_chunks(padded):
    tiles = padded // 256
    out, lo = [], 0
    while tiles:
        take = 4 if tiles % 3 else 3
        take = min(take, tiles)
        out.append((lo, take * 256))
        lo += take * 256
        tiles -= take
    return tuple(out)


def head_logits(hn, emb, labels, vocab, block):
    n, d = hn.shape
    padded = emb.shape[0]
    return pl.pallas_call(
        functools.partial(logits_kernel, make_chunks(padded), vocab),
        grid=(n // block,),
        in_specs=[pl.BlockSpec((block, d), lambda i: (i, 0)),
                  pl.BlockSpec((padded, d), lambda i: (0, 0), pipeline_mode=pl.Buffered(1)),
                  pl.BlockSpec((block, 1), lambda i: (i, 0))],
        out_specs=[pl.BlockSpec((block, padded), lambda i: (i, 0)), pl.BlockSpec((block, 128), lambda i: (i, 0))],
        out_shape=[jax.ShapeDtypeStruct((n, padded), F32), jax.ShapeDtypeStruct((n, 128), F32)],
        compiler_params=pltpu.CompilerParams(vmem_limit_bytes=VMEM_LIMIT),
        cost_estimate=pl.CostEstimate(flops=2 * n * d * padded, bytes_accessed=4 * n * padded, transcendentals=n * padded),
        name="head_logits",
    )(hn, emb, labels)


def head_grads(z, hn, emb, stats, labels, vocab, inv_n, block):
    n, d = hn.shape
    padded = emb.shape[0]
    return pl.pallas_call(
        functools.partial(grads_kernel, make_chunks(padded), vocab, inv_n),
        grid=(n // block,),
        in_specs=[pl.BlockSpec((block, padded), lambda i: (i, 0)),
                  pl.BlockSpec((block, d), lambda i: (i, 0)),
                  pl.BlockSpec((padded, d), lambda i: (0, 0), pipeline_mode=pl.Buffered(1)),
                  pl.BlockSpec((block, 2), lambda i: (i, 0)),
                  pl.BlockSpec((block, 1), lambda i: (i, 0))],
        out_specs=[pl.BlockSpec((block, d), lambda i: (i, 0)),
                   pl.BlockSpec((padded, d), lambda i: (0, 0), pipeline_mode=pl.Buffered(1))],
        out_shape=[jax.ShapeDtypeStruct((n, d), F32), jax.ShapeDtypeStruct((padded, d), F32)],
        compiler_params=pltpu.CompilerParams(vmem_limit_bytes=VMEM_LIMIT),
        cost_estimate=pl.CostEstimate(flops=4 * n * d * padded, bytes_accessed=4 * n * padded, transcendentals=n * padded),
        name="head_grads",
    )(z, hn, emb, stats, labels)


def mlp_forward(x_emb, gain_in, w_gate, w_up, w_down):
    normed_in, norm_in_back = jax.vjp(lambda values: rms_scale(values, gain_in), x_emb)
    normed_bf = normed_in.astype(BF)
    gate_f = jnp.dot(normed_bf, w_gate, preferred_element_type=F32).astype(BF).astype(F32)
    up_f = jnp.dot(normed_bf, w_up, preferred_element_type=F32).astype(BF).astype(F32)
    gate_sig = jax.nn.sigmoid(gate_f)
    silu_gate = gate_f * gate_sig
    act_bf = (silu_gate * up_f).astype(BF)
    mlp_out = jnp.dot(act_bf, w_down, preferred_element_type=F32).astype(BF)
    h_res = x_emb + mlp_out.astype(F32)
    return h_res, (norm_in_back, normed_bf, gate_f, up_f, gate_sig, silu_gate, act_bf)


def mlp_backward(d_hidden, saved, w_gate, w_up, w_down):
    norm_in_back, normed_bf, gate_f, up_f, gate_sig, silu_gate, act_bf = saved
    d_mlp = d_hidden.astype(BF)
    d_act = jnp.einsum("td,fd->tf", d_mlp, w_down, preferred_element_type=F32)
    grad_down = jnp.einsum("tf,td->fd", act_bf, d_mlp, preferred_element_type=F32)
    d_gate = (d_act * up_f * (gate_sig * (1.0 + gate_f * (1.0 - gate_sig)))).astype(BF)
    d_up = (d_act * silu_gate).astype(BF)
    grad_gate = jnp.einsum("td,tf->df", normed_bf, d_gate, preferred_element_type=F32)
    grad_up = jnp.einsum("td,tf->df", normed_bf, d_up, preferred_element_type=F32)
    d_normed = jnp.einsum("tf,df->td", d_gate, w_gate, preferred_element_type=F32) + jnp.einsum("tf,df->td", d_up, w_up, preferred_element_type=F32)
    d_x = d_hidden + norm_in_back(d_normed)[0]
    return d_x, grad_gate, grad_up, grad_down


HN_PARTS = ((0, 176), (176, 176), (352, 160))
STAT_PARTS = ((0, 8), (8, 8), (16, 8))


def solution(mesh):
    tok_spec = P("fsdp", None)
    row_spec = P(AXES, None)
    weight_spec = P("fsdp", None)

    def device_step(tok_ids, tok_labels, table_shard, gate_shard, up_shard, down_shard, gain_in, gain_out):
        m_idx = lax.axis_index("model")
        f_idx = lax.axis_index("fsdp")
        me = m_idx * 4 + f_idx
        vocab, width = table_shard.shape
        own = tok_ids.shape[0] * tok_ids.shape[1] // 4
        num_tokens = own * 16

        def full_weight(shard):
            rows = shard.shape[0] // 4
            piece = lax.dynamic_slice_in_dim(shard, m_idx * rows, rows, axis=0)
            return lax.all_gather(piece, ("fsdp", "model"), axis=0, tiled=True)

        w_gate, w_up, w_down = full_weight(gate_shard), full_weight(up_shard), full_weight(down_shard)
        tokens = lax.all_gather(jnp.stack([tok_ids.reshape(-1), tok_labels.reshape(-1)]), "fsdp", axis=0)
        tokens = tokens.reshape(4, 2, 4, own).transpose(1, 2, 0, 3).reshape(2, 16, own)
        ids, labels = tokens[0], tokens[1].reshape(num_tokens)
        my_ids = lax.dynamic_slice_in_dim(ids, me, 1, axis=0)[0]

        mine = (ids // vocab) == me
        place = lax.broadcasted_iota(jnp.int32, ids.shape, 1)
        picked = lax.sort(jnp.where(mine, place, place + own), dimension=1)
        owner = my_ids // vocab
        owner_hot = (owner[:, None] == jnp.arange(16, dtype=jnp.int32)[None, :])
        counts = jnp.cumsum(owner_hot.astype(jnp.int32), axis=0)
        rank = jnp.sum(jnp.where(owner_hot, counts, 0), axis=1) - 1
        hot_all = (ids // vocab)[:, :, None] == jnp.arange(16, dtype=jnp.int32)
        most = jnp.max(jnp.sum(hot_all.astype(jnp.int32), axis=1))
        rounds = (most + ROUND_ROWS - 1) // ROUND_ROWS

        def served(r):
            pos = lax.dynamic_slice(jnp.pad(picked, ((0, 0), (0, ROUND_ROWS)), constant_values=2 * own), (0, r * ROUND_ROWS), (16, ROUND_ROWS))
            valid = pos < own
            safe = jnp.where(valid, pos, 0)
            row = jnp.take_along_axis(ids, safe, axis=1) - me * vocab
            return valid, jnp.where(valid, row, 0)

        def lookup_round(state):
            r, x = state
            _, row = served(r)
            sent = jnp.take(table_shard, row.reshape(-1), axis=0)
            got = lax.all_to_all(sent, AXES, split_axis=0, concat_axis=0, tiled=True)
            at = rank - r * ROUND_ROWS
            now = (at >= 0) & (at < ROUND_ROWS)
            fetched = jnp.take(got, jnp.where(now, owner * ROUND_ROWS + at, 0), axis=0)
            return r + 1, jnp.where(now[:, None], fetched, x)

        _, x_rows = lax.while_loop(lambda s: s[0] < rounds, lookup_round, (jnp.int32(0), jnp.zeros((own, width), BF)))
        x_emb = x_rows.astype(F32)

        h_res, saved = mlp_forward(x_emb, gain_in, w_gate, w_up, w_down)
        hn_f, norm_out_back = jax.vjp(lambda values: rms_scale(values, gain_out), h_res)
        hn_bf = gather_all(hn_f.astype(BF), HN_PARTS, 0)

        padded = (vocab + 255) // 256 * 256
        emb = jnp.pad(table_shard, ((0, padded - vocab), (0, 0)))
        loc_labels = (labels - me * vocab)
        in_here = (loc_labels >= 0) & (loc_labels < vocab)
        lab_col = jnp.where(in_here, loc_labels, -1).reshape(num_tokens, 1)
        z, local_stats = head_logits(hn_bf, emb, lab_col, vocab, 512)
        packed = local_stats[:, :3].T.reshape(24, num_tokens // 8)
        all_stats = gather_all(packed, STAT_PARTS, 1).reshape(16, 3, num_tokens)
        tops = all_stats[:, 0]
        row_max = jnp.max(tops, axis=0)
        sum_exp = jnp.sum(all_stats[:, 1] * jnp.exp(tops - row_max[None, :]), axis=0)
        label_logit = jnp.sum(all_stats[:, 2], axis=0)
        loss = jnp.sum(row_max + jnp.log(sum_exp) - label_logit) / num_tokens
        stat_cols = jnp.stack([row_max, sum_exp], axis=1)
        dhn_part, d_head = head_grads(z, hn_bf, emb, stat_cols, lab_col, vocab, 1.0 / num_tokens, 256)

        hn_views = tuple((0, count, lambda m, f, lo=lo: (m * 4 + f) * own + lo) for lo, count in HN_PARTS)
        shapes = [(count, width) for _, count in HN_PARTS]
        d_hn = jnp.concatenate(reduce_all([dhn_part], hn_views, shapes, shapes, None, 2), axis=0)
        d_hidden = norm_out_back(d_hn)[0]
        d_x, g_gate, g_up, g_down = mlp_backward(d_hidden, saved, w_gate, w_up, w_down)

        def grad_round(state):
            r, grad = state
            at = rank - r * ROUND_ROWS
            now = (at >= 0) & (at < ROUND_ROWS)
            slot = jnp.where(now, owner * ROUND_ROWS + at, 16 * ROUND_ROWS)
            source = jnp.zeros((16 * ROUND_ROWS + 1,), jnp.int32).at[slot].set(jnp.arange(own, dtype=jnp.int32))[:-1]
            sent = jnp.take(d_x, source, axis=0)
            got = lax.all_to_all(sent, AXES, split_axis=0, concat_axis=0, tiled=True)
            valid, row = served(r)
            valid, row = valid.reshape(-1), row.reshape(-1)
            return r + 1, grad.at[row].add(jnp.where(valid[:, None], got, 0.0))

        _, grad_table = lax.while_loop(lambda s: s[0] < rounds, grad_round, (jnp.int32(0), d_head[:vocab]))

        g_rows, d_rows = w_gate.shape[0] // 16, w_down.shape[0] // 16
        views = (
            (0, g_rows, lambda m, f: f * (4 * g_rows) + m * g_rows),
            (1, g_rows, lambda m, f: f * (4 * g_rows) + m * g_rows),
            (2, d_rows, lambda m, f: f * (4 * d_rows) + m * d_rows),
        )
        pieces = [(g_rows, w_gate.shape[1]), (g_rows, w_gate.shape[1]), (d_rows, w_down.shape[1])]
        grad_gate, grad_up, grad_down = reduce_all(
            [g_gate, g_up, g_down], views, [(4 * r, c) for r, c in pieces], pieces, True, 3)
        return loss, grad_table, grad_gate, grad_up, grad_down

    return jax.shard_map(device_step, mesh=mesh, in_specs=(tok_spec, tok_spec, row_spec, weight_spec, weight_spec, weight_spec, P(), P()), out_specs=(P(), row_spec, weight_spec, weight_spec, weight_spec), check_vma=False)
```

```python
import functools

import jax
import jax.numpy as jnp
from jax import lax
from jax.experimental import pallas as pl
from jax.experimental.pallas import tpu as pltpu
from jax.sharding import PartitionSpec as P

EPS = 1e-6
NT = (((1,), (1,)), ((), ()))
TN = (((0,), (0,)), ((), ()))
MESH = pl.DeviceIdType.MESH
AXES = ("model", "fsdp")
BF = jnp.bfloat16
F32 = jnp.float32
ROUND_ROWS = 56
VMEM_LIMIT = 66977792
ANY = pl.BlockSpec(memory_space=pl.ANY)
DMA = pltpu.SemaphoreType.DMA
DIMS = (1, 2, 4)
CHUNK = 8


def rms_scale(values, gain_vec):
    mean_sq = jnp.mean(values * values, axis=-1, keepdims=True)
    return values * lax.rsqrt(mean_sq + EPS) * gain_vec


def my_place():
    m = lax.axis_index("model")
    f = lax.axis_index("fsdp")
    return (f // 2, m % 2, m // 2, f % 2)


def flipped(place, bits, core=False):
    x, y, z, c = place
    if bits & 1:
        x = 1 - x
    if bits & 2:
        y = 1 - y
    if bits & 4:
        z = 1 - z
    if core:
        c = 1 - c
    return (x, y, z, c)


def mesh_id(place):
    x, y, z, c = place
    return (2 * z + y, 2 * x + c)


def greet(place, bit_list, core):
    barrier = pltpu.get_barrier_semaphore()
    peers = [flipped(place, b) for b in bit_list] + ([flipped(place, 0, True)] if core else [])
    for peer in peers:
        pl.semaphore_signal(barrier, inc=1, device_id=mesh_id(peer), device_id_type=MESH)
    pl.semaphore_wait(barrier, len(peers))


ORDERS = (DIMS, DIMS[1:] + DIMS[:1], DIMS[2:] + DIMS[:2])


def subsets(bits):
    out = [0]
    for b in bits:
        out = out + [o | b for o in out]
    return out


def device_of(place):
    m, f = mesh_id(place)
    return m * 4 + f


class Gather:
    def __init__(self, me, parts, rows, in_ref, out_ref, local_sem, send_sem, recv_sem, core_send, core_recv):
        self.me, self.parts, self.rows, self.in_ref, self.out_ref = me, parts, rows, in_ref, out_ref
        self.local_sem, self.sems, self.core_sems = local_sem, (send_sem, recv_sem), (core_send, core_recv)

    def part(self, place, color):
        lo, count = self.parts[color]
        return self.out_ref.at[pl.ds(pl.multiple_of(device_of(place) * self.rows + lo, CHUNK), count)]

    def copy(self, color, bits, core_src, peer, sems, k):
        lo, count = self.parts[color]
        dst = self.part(flipped(self.me, bits, core_src), color)
        src = dst if bits or core_src else self.in_ref.at[pl.ds(lo, count)]
        send, recv = sems
        return pltpu.make_async_remote_copy(
            src_ref=src, dst_ref=dst, send_sem=send.at[k], recv_sem=recv.at[k],
            device_id=mesh_id(peer), device_id_type=MESH)

    def chip(self, color, stage, held, arrival=False):
        order = ORDERS[color]
        k = color * CHUNK + (1 << stage) + subsets(order[:stage]).index(held)
        bits = held | order[stage] if arrival else held
        return self.copy(color, bits, False, flipped(self.me, order[stage]), self.sems, k)

    def core(self, color, bits, arrival=False):
        return self.copy(color, bits, arrival, flipped(self.me, 0, True), self.core_sems, color * CHUNK + bits)

    def local(self):
        at = pl.ds(pl.multiple_of(device_of(self.me) * self.rows, CHUNK), self.rows)
        return pltpu.make_async_copy(self.in_ref, self.out_ref.at[at], self.local_sem)

    def begin(self):
        greet(self.me, DIMS, True)
        self.local().start()
        for stage in range(3):
            for color in range(3):
                self.chip(color, stage, 0).start()
        for color in range(3):
            self.core(color, 0).start()

    def arrive(self, stage, index):
        for color in range(3):
            order = ORDERS[color]
            held = subsets(order[:stage])[index]
            self.chip(color, stage, held, True).wait_recv()
            bits = held | order[stage]
            for later in range(stage + 1, 3):
                self.chip(color, later, bits).start()
            self.core(color, bits).start()

    def core_arrive(self, bits):
        for color in range(3):
            self.core(color, bits, True).wait_recv()

    def finish(self):
        for color in range(3):
            for stage in range(3):
                for held in subsets(ORDERS[color][:stage]):
                    self.chip(color, stage, held).wait_send()
            for bits in range(8):
                self.core(color, bits).wait_send()
        self.local().wait()


def gather_sems():
    return [DMA] + [DMA((3 * CHUNK,))] * 4


def gather_kernel(parts, rows, *refs):
    g = Gather(my_place(), parts, rows, *refs)
    g.begin()
    for stage in range(3):
        for index in range(1 << stage):
            g.arrive(stage, index)
    for bits in range(8):
        g.core_arrive(bits)
    g.finish()


def gather_all(values, parts, collective_id):
    rows, width = values.shape
    return pl.pallas_call(
        functools.partial(gather_kernel, parts, rows),
        out_shape=jax.ShapeDtypeStruct((16 * rows, width), values.dtype),
        in_specs=[ANY], out_specs=ANY, scratch_shapes=gather_sems(),
        compiler_params=pltpu.CompilerParams(collective_id=collective_id, has_side_effects=True),
        name="gather_stats",
    )(values)


BLOCK_ORDER = (7, 6, 5, 3, 4, 2, 1, 0)


def add_rows(dst, slot_a, src, slot_b, lo, rows, chunk):
    def body(i, carry):
        at = pl.ds(pl.multiple_of(lo + i * chunk, 8), chunk)
        dst[slot_a, at, :] = dst[slot_a, at, :] + src[slot_b, at, :]
        return carry

    lax.fori_loop(0, rows // chunk, body, 0)


def stage_of(color, bits):
    order = ORDERS[color]
    for s in range(3):
        if bits & order[s]:
            return s
    return 3


def box_slot(color, stage, bits):
    rest = subsets(ORDERS[color][stage + 1:])
    return (0, 4, 6)[stage] + rest.index(bits)


def back_kernel(chunks, vocab, inv_n, parts, half, z_ref, emb_ref, st_ref, lab_ref, dz_ref, out_ref,
                acc, pairs, boxes, core_send, core_recv, send_sem, recv_sem, out_sem):
    i = pl.program_id(0)
    me = my_place()

    @pl.when(i == 0)
    def _():
        greet(me, DIMS, True)

    def core_copy(t):
        return pltpu.make_async_remote_copy(
            src_ref=acc.at[8 + t % 2], dst_ref=pairs.at[7 - t], send_sem=core_send.at[t], recv_sem=core_recv.at[t],
            device_id=mesh_id(flipped(me, 0, True)), device_id_type=MESH)

    def chip_copy(color, stage, bits):
        lo, count = parts[color]
        slot = box_slot(color, stage, bits & ~ORDERS[color][stage])
        k = color * 8 + slot
        return pltpu.make_async_remote_copy(
            src_ref=acc.at[bits, pl.ds(lo, count)], dst_ref=boxes.at[slot, pl.ds(lo, count)],
            send_sem=send_sem.at[k], recv_sem=recv_sem.at[k],
            device_id=mesh_id(flipped(me, ORDERS[color][stage])), device_id_type=MESH)

    for t in range(2, 8):
        @pl.when(i == 4 * t)
        def _(t=t):
            core_copy(t - 2).wait_send()

    lab = lab_ref[...]
    top = st_ref[:, 0:1]
    inv_sum = 1.0 / st_ref[:, 1:2]
    total = None
    for lo, count in chunks:
        z = z_ref[:, lo:lo + count]
        p = jnp.exp(z - top) * inv_sum
        col = lax.broadcasted_iota(jnp.int32, z.shape, 1) + lo
        p = jnp.where(col == lab, p - 1.0, p) * inv_n
        if lo + count > vocab:
            p = jnp.where(col < vocab, p, 0.0)
        dz = p.astype(BF)
        dz_ref[:, lo:lo + count] = dz
        part = jnp.dot(dz, emb_ref[lo:lo + count, :], preferred_element_type=F32)
        total = part if total is None else total + part
    t_now = i // 4
    own = (i // 2) % 2
    slot_now = own * (7 - t_now) + (1 - own) * (8 + t_now % 2)
    acc[slot_now, pl.ds(pl.multiple_of((i % 2) * half, half), half), :] = total

    for t in range(8):
        bits = 7 - t

        @pl.when(i == 4 * t + 1)
        def _(t=t):
            core_copy(t).start()

        @pl.when(i == 4 * t + 3)
        def _(t=t, bits=bits):
            core_copy(t).wait_recv()
            for color in range(3):
                lo, count = parts[color]
                add_rows(acc, bits, pairs, bits, lo, count, 16)
                mine = stage_of(color, bits)
                for s in range(mine):
                    chip_copy(color, s, bits | ORDERS[color][s]).wait_recv()
                    add_rows(acc, bits, boxes, box_slot(color, s, bits), lo, count, 16)
                if mine < 3:
                    chip_copy(color, mine, bits).start()

    @pl.when(i == 31)
    def _():
        done = pltpu.make_async_copy(acc.at[0], out_ref, out_sem)
        done.start()
        for t in (6, 7):
            core_copy(t).wait_send()
        for color in range(3):
            for bits in range(1, 8):
                chip_copy(color, stage_of(color, bits), bits).wait_send()
        done.wait()


def head_back(z, emb, stats, labels, parts, vocab, inv_n, collective_id):
    n, padded = z.shape
    d = emb.shape[1]
    rows = n // 16
    half = rows // 2

    def block(i):
        return (device_of(moved(my_place(), 7 - i // 4, 1 - (i // 2) % 2)) * 2 + i % 2, 0)

    return pl.pallas_call(
        functools.partial(back_kernel, make_chunks(padded), vocab, inv_n, parts, half),
        grid=(32,),
        in_specs=[pl.BlockSpec((half, padded), block),
                  pl.BlockSpec((padded, d), lambda i: (0, 0), pipeline_mode=pl.Buffered(1)),
                  pl.BlockSpec((half, 2), block),
                  pl.BlockSpec((half, 1), block)],
        out_specs=[pl.BlockSpec((half, padded), block), ANY],
        out_shape=[jax.ShapeDtypeStruct((n, padded), BF), jax.ShapeDtypeStruct((rows, d), F32)],
        scratch_shapes=[pltpu.VMEM((10, rows, d), F32), pltpu.VMEM((8, rows, d), F32), pltpu.VMEM((7, rows, d), F32),
                        DMA((8,)), DMA((8,)),
                        DMA((24,)), DMA((24,)), DMA],
        compiler_params=pltpu.CompilerParams(collective_id=collective_id, has_side_effects=True, vmem_limit_bytes=VMEM_LIMIT,
                                             ),
        name="head_back",
    )(z, emb, stats, labels)


def tail_kernel(chunks, vocab, views, swap_rows, dz_ref, hn_ref, *refs):
    n_in = max(v[0] for v in views) + 2
    ins, rows_ref = refs[:n_in - 1], refs[n_in - 1]
    de_ref = refs[n_in]
    outs = refs[n_in + 1:n_in + 4]
    back_ref = refs[n_in + 4]
    rest = refs[n_in + 5:]
    accs, pairs, boxes = rest[0:3], rest[3:6], rest[6:9]
    (load_sem, core_send, core_recv, send_sem, recv_sem, out_sem, sp_send, sp_recv, row_send, row_recv, row_sem) = rest[9:]
    i = pl.program_id(0)
    me = my_place()

    def source(color, place):
        which, rows, start, col, cols = views[color]
        m, f = mesh_id(place)
        return ins[which].at[pl.ds(pl.multiple_of(start(m, f), 8), rows), pl.ds(col, cols)]

    def load(color, bits):
        return pltpu.make_async_copy(source(color, flipped(me, bits)), accs[color].at[bits], load_sem.at[color * 8 + bits])

    def core_copy(color, bits):
        k = color * 8 + bits
        return pltpu.make_async_remote_copy(
            src_ref=source(color, flipped(me, bits, True)), dst_ref=pairs[color].at[bits],
            send_sem=core_send.at[k], recv_sem=core_recv.at[k],
            device_id=mesh_id(flipped(me, 0, True)), device_id_type=MESH)

    def chip_copy(color, stage, bits):
        slot = box_slot(color, stage, bits & ~ORDERS[color][stage])
        k = color * 8 + slot
        return pltpu.make_async_remote_copy(
            src_ref=accs[color].at[bits], dst_ref=boxes[color].at[slot],
            send_sem=send_sem.at[k], recv_sem=recv_sem.at[k],
            device_id=mesh_id(flipped(me, ORDERS[color][stage])), device_id_type=MESH)

    def row_copy(bits, core):
        k = 2 * bits + int(core)
        peer = flipped(me, bits, core)
        return pltpu.make_async_remote_copy(
            src_ref=rows_ref.at[pl.ds(pl.multiple_of(device_of(peer) * swap_rows, 8), swap_rows)],
            dst_ref=back_ref.at[pl.ds(pl.multiple_of(device_of(me) * swap_rows, 8), swap_rows)],
            send_sem=row_send.at[k], recv_sem=row_recv.at[k], device_id=mesh_id(peer), device_id_type=MESH)

    def row_arrival(bits, core):
        k = 2 * bits + int(core)
        peer = flipped(me, bits, core)
        dst = back_ref.at[pl.ds(pl.multiple_of(device_of(peer) * swap_rows, 8), swap_rows)]
        return pltpu.make_async_remote_copy(
            src_ref=dst, dst_ref=dst, send_sem=row_send.at[k], recv_sem=row_recv.at[k],
            device_id=mesh_id(peer), device_id_type=MESH)

    own_rows = pl.ds(pl.multiple_of(device_of(me) * swap_rows, 8), swap_rows)
    row_local = pltpu.make_async_copy(rows_ref.at[own_rows], back_ref.at[own_rows], row_sem)
    others = [(b, c) for b in BLOCK_ORDER for c in (False, True) if b or c]

    halves = ((2, 4), (4, 2))

    def target(color, place, half):
        rows = views[color][1]
        m, f = mesh_id(place)
        return outs[color].at[pl.ds(pl.multiple_of(m * rows + half * (rows // 2), 8), rows // 2)]

    def spread_copy(color, half, step, bits):
        rows = views[color][1]
        first, second = halves[half]
        src = accs[color].at[0, pl.ds(half * (rows // 2), rows // 2)] if bits == 0 else target(color, flipped(me, bits), half)
        k = (color * 2 + half) * 3 + step
        return pltpu.make_async_remote_copy(
            src_ref=src, dst_ref=target(color, flipped(me, bits), half),
            send_sem=sp_send.at[k], recv_sem=sp_recv.at[k],
            device_id=mesh_id(flipped(me, first if step == 0 else second)), device_id_type=MESH)

    def out_copy(color):
        rows = views[color][1]
        m, f = mesh_id(me)
        return pltpu.make_async_copy(accs[color].at[0], outs[color].at[pl.ds(pl.multiple_of(m * rows, 8), rows)], out_sem.at[color])

    @pl.when(i == 0)
    def _():
        barrier = pltpu.get_barrier_semaphore()
        for bits, core in others:
            pl.semaphore_signal(barrier, inc=1, device_id=mesh_id(flipped(me, bits, core)), device_id_type=MESH)
        pl.semaphore_wait(barrier, len(others))
        for bits in BLOCK_ORDER:
            for color in range(3):
                core_copy(color, bits).start()
                load(color, bits).start()
        row_local.start()
        de_ref[...] = jnp.zeros_like(de_ref)

    hn = hn_ref[...]
    for lo, count in chunks:
        keep = min(count, vocab - lo)
        part = lax.dot_general(dz_ref[:, lo:lo + count], hn, TN, preferred_element_type=F32)
        de_ref[lo:lo + keep, :] += part[:keep]

    for t in range(8):
        bits = BLOCK_ORDER[t]

        @pl.when(i == t)
        def _(bits=bits):
            for color in range(3):
                rows = views[color][1]
                load(color, bits).wait()
                core_copy(color, bits).wait_recv()
                add_rows(accs[color], bits, pairs[color], bits, 0, rows, 8)
                if stage_of(color, bits) == 0:
                    chip_copy(color, 0, bits).start()

    @pl.when(i == 8)
    def _():
        for bits, core in others:
            row_copy(bits, core).start()

    def arrivals(stage, index):
        for color in range(3):
            order = ORDERS[color]
            bits = sorted(subsets(order[stage + 1:]), key=lambda b: stage_of(color, b))[index]
            slot = box_slot(color, stage, bits)
            chip_copy(color, stage, bits | order[stage]).wait_recv()
            add_rows(accs[color], bits, boxes[color], slot, 0, views[color][1], 8)
            if stage_of(color, bits) == stage + 1 and stage < 2:
                chip_copy(color, stage + 1, bits).start()

    for step, (stage, index) in enumerate([(s, j) for s in range(2) for j in range(4 >> s)]):
        @pl.when(i == 9 + step)
        def _(stage=stage, index=index):
            arrivals(stage, index)

    @pl.when(i == 15)
    def _():
        arrivals(2, 0)
        for color in range(3):
            out_copy(color).start()
            for half in range(2):
                for step in range(2):
                    spread_copy(color, half, step, 0).start()
        for color in range(3):
            for half in range(2):
                spread_copy(color, half, 0, halves[half][0]).wait_recv()
                spread_copy(color, half, 2, halves[half][0]).start()
        for bits, core in others:
            row_arrival(bits, core).wait_recv()
        for color in range(3):
            for half in range(2):
                first, second = halves[half]
                spread_copy(color, half, 1, second).wait_recv()
                spread_copy(color, half, 2, first | second).wait_recv()
        for color in range(3):
            for bits in range(8):
                core_copy(color, bits).wait_send()
                if bits:
                    chip_copy(color, stage_of(color, bits), bits).wait_send()
            for half in range(2):
                for step in range(3):
                    spread_copy(color, half, step, halves[half][0] if step == 2 else 0).wait_send()
            out_copy(color).wait()
        for bits, core in others:
            row_copy(bits, core).wait_send()
        row_local.wait()


def tail_all(dz, hn, arrays, rows, views, piece_shapes, vocab, swap_rows, collective_id):
    n, padded = dz.shape
    d = hn.shape[1]
    block = n // 16
    scratch = []
    for count in (8, 8, 7):
        for shape in piece_shapes:
            scratch.append(pltpu.VMEM((count,) + shape, F32))
    sems = [DMA((24,))] * 5 + [DMA((3,))] + [DMA((18,))] * 2 + [DMA((16,))] * 2 + [DMA]
    return pl.pallas_call(
        functools.partial(tail_kernel, make_chunks(padded), vocab, views, swap_rows),
        grid=(16,),
        in_specs=[pl.BlockSpec((block, padded), lambda i: (i, 0)), pl.BlockSpec((block, d), lambda i: (i, 0))]
        + [ANY] * (len(arrays) + 1),
        out_specs=[pl.BlockSpec((vocab, d), lambda i: (0, 0), pipeline_mode=pl.Buffered(1))] + [ANY] * 4,
        out_shape=[jax.ShapeDtypeStruct((vocab, d), F32)]
        + [jax.ShapeDtypeStruct((4 * r, c), F32) for r, c in piece_shapes]
        + [jax.ShapeDtypeStruct(rows.shape, F32)],
        scratch_shapes=scratch + sems,
        compiler_params=pltpu.CompilerParams(collective_id=collective_id, has_side_effects=True, vmem_limit_bytes=VMEM_LIMIT,
                                             ),
        name="tail_all",
    )(dz, hn, *arrays, rows)


def moved(place, bits, core):
    x, y, z, c = place
    flips = (bits % 2, (bits // 2) % 2, bits // 4, core)
    return tuple(p + q - 2 * p * q for p, q in zip((x, y, z, c), flips))


ARRIVALS = {1: ((0, 0), (1, 0), (2, 0)), 2: ((1, 1),), 3: ((2, 1),), 4: ((2, 2),), 7: ((2, 3),)}


def logits_kernel(chunks, vocab, parts, rows, in_ref, emb_ref, lab_ref, all_ref, z_ref, st_ref, blocks, load_sem, *sems):
    i = pl.program_id(0)
    me = my_place()
    g = Gather(me, parts, rows, in_ref, all_ref, *sems)

    def load(step):
        at = device_of(moved(me, step // 2, step % 2)) * rows
        return pltpu.make_async_copy(all_ref.at[pl.ds(pl.multiple_of(at, CHUNK), rows)], blocks.at[step % 2], load_sem.at[step % 2])

    first = pltpu.make_async_copy(in_ref, blocks.at[0], load_sem.at[0])

    @pl.when(i == 0)
    def _():
        g.begin()
        first.start()

    for step, groups in ARRIVALS.items():
        @pl.when(i == step)
        def _(groups=groups):
            for stage, index in groups:
                g.arrive(stage, index)

    for bits in range(8):
        @pl.when(i == 2 * bits)
        def _(bits=bits):
            g.core_arrive(bits)

    @pl.when(i < 15)
    def _():
        load(i + 1).start()

    load(i).wait()
    hn = blocks[i % 2]
    lab = lab_ref[...]
    top = lab_z = total = None
    for lo, count in chunks:
        z = lax.dot_general(hn, emb_ref[lo:lo + count, :], NT, preferred_element_type=F32)
        z_ref[:, lo:lo + count] = z
        col = lax.broadcasted_iota(jnp.int32, z.shape, 1) + lo
        picked = jnp.sum(jnp.where(col == lab, z, 0.0), axis=1, keepdims=True)
        if lo + count > vocab:
            z = jnp.where(col < vocab, z, -jnp.inf)
        peak = jnp.max(z, axis=1, keepdims=True)
        top = peak if top is None else jnp.maximum(top, peak)
        lab_z = picked if lab_z is None else lab_z + picked
    for lo, count in chunks:
        z = z_ref[:, lo:lo + count]
        e = jnp.exp(z - top)
        if lo + count > vocab:
            col = lax.broadcasted_iota(jnp.int32, z.shape, 1) + lo
            e = jnp.where(col < vocab, e, 0.0)
        part = jnp.sum(e, axis=1, keepdims=True)
        total = part if total is None else total + part
    lane = lax.broadcasted_iota(jnp.int32, (rows, 128), 1)
    packed = jnp.where(lane == 0, top, jnp.where(lane == 1, total, lab_z))
    st_ref[...] = packed.T[:CHUNK]

    @pl.when(i == 15)
    def _():
        g.finish()


def make_chunks(padded):
    units = padded // 128
    count = (units + 7) // 8
    out, lo = [], 0
    for k in range(count, 0, -1):
        take = min(units, ((units + k - 1) // k + 1) // 2 * 2)
        out.append((lo, take * 128))
        lo += take * 128
        units -= take
    return tuple(out)


def head_logits(hn, emb, labels, parts, vocab, collective_id):
    rows, d = hn.shape
    n = 16 * rows
    padded = emb.shape[0]

    def block(i):
        return (device_of(moved(my_place(), i // 2, i % 2)), 0)

    return pl.pallas_call(
        functools.partial(logits_kernel, make_chunks(padded), vocab, parts, rows),
        grid=(16,),
        in_specs=[ANY, pl.BlockSpec((padded, d), lambda i: (0, 0), pipeline_mode=pl.Buffered(1)), pl.BlockSpec((rows, 1), block)],
        out_specs=[ANY, pl.BlockSpec((rows, padded), block), pl.BlockSpec((CHUNK, rows), block)],
        out_shape=[jax.ShapeDtypeStruct((n, d), BF), jax.ShapeDtypeStruct((n, padded), F32),
                   jax.ShapeDtypeStruct((16 * CHUNK, rows), F32)],
        scratch_shapes=[pltpu.VMEM((2, rows, d), BF), DMA((2,))] + gather_sems(),
        compiler_params=pltpu.CompilerParams(collective_id=collective_id, has_side_effects=True, vmem_limit_bytes=VMEM_LIMIT),
        name="head_logits",
    )(hn, emb, labels)


def mlp_forward(x_emb, gain_in, w_in, w_down):
    normed_in, norm_in_back = jax.vjp(lambda values: rms_scale(values, gain_in), x_emb)
    normed_bf = normed_in.astype(BF)
    both = jnp.dot(normed_bf, w_in, preferred_element_type=F32).astype(BF)
    hidden = w_down.shape[0]
    gate_f = both[:, :hidden].astype(F32)
    up_f = both[:, hidden:].astype(F32)
    gate_sig = jax.nn.sigmoid(gate_f)
    silu_gate = gate_f * gate_sig
    act_bf = (silu_gate * up_f).astype(BF)
    mlp_out = jnp.dot(act_bf, w_down, preferred_element_type=F32).astype(BF)
    h_res = x_emb + mlp_out.astype(F32)
    return h_res, (norm_in_back, normed_bf, gate_f, up_f, gate_sig, silu_gate, act_bf)


def mlp_backward(d_hidden, saved, w_in, w_down):
    norm_in_back, normed_bf, gate_f, up_f, gate_sig, silu_gate, act_bf = saved
    d_mlp = d_hidden.astype(BF)
    d_act = jnp.einsum("td,fd->tf", d_mlp, w_down, preferred_element_type=F32)
    grad_down = jnp.einsum("tf,td->fd", act_bf, d_mlp, preferred_element_type=F32)
    d_gate = (d_act * up_f * (gate_sig * (1.0 + gate_f * (1.0 - gate_sig)))).astype(BF)
    d_up = (d_act * silu_gate).astype(BF)
    d_both = jnp.concatenate([d_gate, d_up], axis=1)
    grad_in = jnp.einsum("td,tf->df", normed_bf, d_both, preferred_element_type=F32)
    d_normed = jnp.einsum("tf,df->td", d_both, w_in, preferred_element_type=F32)
    d_x = d_hidden + norm_in_back(d_normed)[0]
    return d_x, grad_in, grad_down


HN_PARTS = ((0, 176), (176, 176), (352, 160))
STAT_PARTS = ((0, 8), (8, 8), (16, 8))


def solution(mesh):
    tok_spec = P("fsdp")
    row_spec = P(AXES)
    weight_spec = P("fsdp")

    def device_step(tok_ids, tok_labels, table_shard, gate_shard, up_shard, down_shard, gain_in, gain_out):
        m_idx = lax.axis_index("model")
        f_idx = lax.axis_index("fsdp")
        me = m_idx * 4 + f_idx
        vocab, width = table_shard.shape
        own = tok_ids.shape[0] * tok_ids.shape[1] // 4
        num_tokens = own * 16

        def full_weight(shard):
            rows = shard.shape[0] // 4
            piece = lax.dynamic_slice_in_dim(shard, m_idx * rows, rows, axis=0)
            return lax.all_gather(piece, ("fsdp", "model"), axis=0, tiled=True)

        w_in = full_weight(jnp.concatenate([gate_shard, up_shard], axis=1))
        w_down = full_weight(down_shard)
        tokens = lax.all_gather(jnp.stack([tok_ids.reshape(-1), tok_labels.reshape(-1)]), "fsdp", axis=0)
        tokens = tokens.reshape(4, 2, 4, own).transpose(1, 2, 0, 3).reshape(2, 16, own)
        ids, labels = tokens[0], tokens[1].reshape(num_tokens)
        my_ids = lax.dynamic_slice_in_dim(ids, me, 1, axis=0)[0]

        base = vocab * 16
        place = lax.broadcasted_iota(jnp.int32, ids.shape, 1)
        mine = (ids // vocab) == me
        owner = my_ids // vocab
        owner_hot = owner[None, :] == jnp.arange(16, dtype=jnp.int32)[:, None]
        keys = jnp.concatenate([
            jnp.where(mine, place, place + own) * base + ids,
            jnp.where(owner_hot, place, place + own) * base], axis=0)
        keys = lax.sort(keys, dimension=1)
        keys = jnp.pad(keys, ((0, 0), (0, ROUND_ROWS)), constant_values=own * base)
        rank = jnp.sum(jnp.where(owner_hot, jnp.cumsum(owner_hot.astype(jnp.int32), axis=1), 0), axis=0) - 1
        hot_all = (ids // vocab)[:, None, :] == jnp.arange(16, dtype=jnp.int32)[None, :, None]
        most = jnp.max(jnp.sum(hot_all.astype(jnp.int32), axis=2))
        rounds = (most + ROUND_ROWS - 1) // ROUND_ROWS

        def round_keys(first, r):
            key = lax.dynamic_slice(keys, (first, r * ROUND_ROWS), (16, ROUND_ROWS)).reshape(-1)
            return key < own * base, key

        def served(r):
            valid, key = round_keys(0, r)
            return valid, jnp.where(valid, key % base - me * vocab, 0)

        def returned(r):
            valid, key = round_keys(16, r)
            return jnp.where(valid, key // base, 0)

        def take_rows(values, rows):
            return jnp.take(values, rows, axis=0)

        def exchange(values):
            return lax.all_to_all(values, AXES, 0, 0, tiled=True)

        def lookup_round(state):
            r, x = state
            _, row = served(r)
            got = exchange(take_rows(table_shard, row))
            at = rank - r * ROUND_ROWS
            now = (at >= 0) & (at < ROUND_ROWS)
            fetched = take_rows(got, jnp.where(now, owner * ROUND_ROWS + at, 0))
            return r + 1, jnp.where(now[:, None], fetched, x)

        _, x_rows = lax.while_loop(lambda s: s[0] < rounds, lookup_round, (jnp.int32(0), jnp.zeros((own, width), BF)))
        x_emb = x_rows.astype(F32)

        h_res, saved = mlp_forward(x_emb, gain_in, w_in, w_down)
        hn_f, norm_out_back = jax.vjp(lambda values: rms_scale(values, gain_out), h_res)
        padded = (vocab + 127) // 128 * 128
        emb = jnp.pad(table_shard, ((0, padded - vocab), (0, 0)))
        loc_labels = labels - me * vocab
        in_here = (loc_labels >= 0) & (loc_labels < vocab)
        lab_col = jnp.where(in_here, loc_labels, -1).reshape(num_tokens, 1)
        hn_bf, z, local_stats = head_logits(hn_f.astype(BF), emb, lab_col, HN_PARTS, vocab, 0)
        packed = local_stats.reshape(16, CHUNK, own)[:, :3].transpose(1, 0, 2).reshape(24, num_tokens // 8)
        all_stats = gather_all(packed, STAT_PARTS, 1).reshape(16, 3, num_tokens)
        tops = all_stats[:, 0]
        row_max = jnp.max(tops, axis=0)
        sum_exp = jnp.sum(all_stats[:, 1] * jnp.exp(tops - row_max[None, :]), axis=0)
        label_logit = jnp.sum(all_stats[:, 2], axis=0)
        loss = jnp.sum(row_max + jnp.log(sum_exp) - label_logit) / num_tokens
        stat_cols = jnp.stack([row_max, sum_exp], axis=1)
        dz, d_hn = head_back(z, emb, stat_cols, lab_col, HN_PARTS, vocab, 1.0 / num_tokens, 2)
        d_hidden = norm_out_back(d_hn)[0]
        d_x, g_in, g_down = mlp_backward(d_hidden, saved, w_in, w_down)

        g_rows, hidden = w_in.shape[0] // 16, w_down.shape[0]
        d_rows = hidden // 16
        views = (
            (0, g_rows, lambda m, f: f * (4 * g_rows) + m * g_rows, 0, hidden),
            (0, g_rows, lambda m, f: f * (4 * g_rows) + m * g_rows, hidden, hidden),
            (1, d_rows, lambda m, f: f * (4 * d_rows) + m * d_rows, 0, width),
        )
        pieces = [(g_rows, hidden), (g_rows, hidden), (d_rows, width)]
        sent = take_rows(d_x, returned(0))
        d_head, grad_gate, grad_up, grad_down, got = tail_all(
            dz, hn_bf, [g_in, g_down], sent, views, pieces, vocab, ROUND_ROWS, 3)

        def add_round(grad, r, got):
            valid, row = served(r)
            return grad.at[row].add(jnp.where(valid[:, None], got, 0.0))

        def grad_round(state):
            r, grad = state
            return r + 1, add_round(grad, r, exchange(take_rows(d_x, returned(r))))

        _, grad_table = lax.while_loop(lambda s: s[0] < rounds, grad_round, (jnp.int32(1), add_round(d_head, 0, got)))
        return loss, grad_table, grad_gate, grad_up, grad_down

    return jax.shard_map(device_step, mesh=mesh, in_specs=(tok_spec, tok_spec, row_spec, weight_spec, weight_spec, weight_spec, P(), P()), out_specs=(P(), row_spec, weight_spec, weight_spec, weight_spec), check_vma=False)
```

```python
import functools

import jax
import jax.numpy as jnp
from jax import lax
from jax.experimental import pallas as pl
from jax.experimental.pallas import tpu as pltpu
from jax.sharding import PartitionSpec as P

EPS = 1e-6
NT = (((1,), (1,)), ((), ()))
TN = (((0,), (0,)), ((), ()))
MESH = pl.DeviceIdType.MESH
AXES = ("model", "fsdp")
BF = jnp.bfloat16
F32 = jnp.float32
ROUND_ROWS = 56
VMEM_LIMIT = 66977792
ANY = pl.BlockSpec(memory_space=pl.ANY)
DMA = pltpu.SemaphoreType.DMA
DIMS = (1, 2, 4)
CHUNK = 8


def rms_scale(values, gain_vec):
    mean_sq = jnp.mean(values * values, axis=-1, keepdims=True)
    return values * lax.rsqrt(mean_sq + EPS) * gain_vec


def my_place():
    m = lax.axis_index("model")
    f = lax.axis_index("fsdp")
    return (f // 2, m % 2, m // 2, f % 2)


def flipped(place, bits, core=False):
    x, y, z, c = place
    if bits & 1:
        x = 1 - x
    if bits & 2:
        y = 1 - y
    if bits & 4:
        z = 1 - z
    if core:
        c = 1 - c
    return (x, y, z, c)


def mesh_id(place):
    x, y, z, c = place
    return (2 * z + y, 2 * x + c)


def greet(place, bit_list, core):
    barrier = pltpu.get_barrier_semaphore()
    peers = [flipped(place, b) for b in bit_list] + ([flipped(place, 0, True)] if core else [])
    for peer in peers:
        pl.semaphore_signal(barrier, inc=1, device_id=mesh_id(peer), device_id_type=MESH)
    pl.semaphore_wait(barrier, len(peers))


ORDERS = (DIMS, DIMS[1:] + DIMS[:1], DIMS[2:] + DIMS[:2])


def subsets(bits):
    out = [0]
    for b in bits:
        out = out + [o | b for o in out]
    return out


def device_of(place):
    m, f = mesh_id(place)
    return m * 4 + f


class Gather:
    def __init__(self, me, parts, rows, in_ref, out_ref, local_sem, send_sem, recv_sem, core_send, core_recv):
        self.me, self.parts, self.rows, self.in_ref, self.out_ref = me, parts, rows, in_ref, out_ref
        self.local_sem, self.sems, self.core_sems = local_sem, (send_sem, recv_sem), (core_send, core_recv)

    def part(self, place, color):
        lo, count = self.parts[color]
        return self.out_ref.at[pl.ds(pl.multiple_of(device_of(place) * self.rows + lo, CHUNK), count)]

    def copy(self, color, bits, core_src, peer, sems, k):
        lo, count = self.parts[color]
        dst = self.part(flipped(self.me, bits, core_src), color)
        src = dst if bits or core_src else self.in_ref.at[pl.ds(lo, count)]
        send, recv = sems
        return pltpu.make_async_remote_copy(
            src_ref=src, dst_ref=dst, send_sem=send.at[k], recv_sem=recv.at[k],
            device_id=mesh_id(peer), device_id_type=MESH)

    def chip(self, color, stage, held, arrival=False):
        order = ORDERS[color]
        k = color * CHUNK + (1 << stage) + subsets(order[:stage]).index(held)
        bits = held | order[stage] if arrival else held
        return self.copy(color, bits, False, flipped(self.me, order[stage]), self.sems, k)

    def core(self, color, bits, arrival=False):
        return self.copy(color, bits, arrival, flipped(self.me, 0, True), self.core_sems, color * CHUNK + bits)

    def local(self):
        at = pl.ds(pl.multiple_of(device_of(self.me) * self.rows, CHUNK), self.rows)
        return pltpu.make_async_copy(self.in_ref, self.out_ref.at[at], self.local_sem)

    def begin(self):
        greet(self.me, DIMS, True)
        self.local().start()
        for stage in range(3):
            for color in range(3):
                self.chip(color, stage, 0).start()
        for color in range(3):
            self.core(color, 0).start()

    def arrive(self, stage, index):
        for color in range(3):
            order = ORDERS[color]
            held = subsets(order[:stage])[index]
            self.chip(color, stage, held, True).wait_recv()
            bits = held | order[stage]
            for later in range(stage + 1, 3):
                self.chip(color, later, bits).start()
            self.core(color, bits).start()

    def core_arrive(self, bits):
        for color in range(3):
            self.core(color, bits, True).wait_recv()

    def finish(self):
        for color in range(3):
            for stage in range(3):
                for held in subsets(ORDERS[color][:stage]):
                    self.chip(color, stage, held).wait_send()
            for bits in range(8):
                self.core(color, bits).wait_send()
        self.local().wait()


def gather_sems():
    return [DMA] + [DMA((3 * CHUNK,))] * 4


def gather_kernel(parts, rows, *refs):
    g = Gather(my_place(), parts, rows, *refs)
    g.begin()
    for stage in range(3):
        for index in range(1 << stage):
            g.arrive(stage, index)
    for bits in range(8):
        g.core_arrive(bits)
    g.finish()


def gather_all(values, parts, collective_id):
    rows, width = values.shape
    return pl.pallas_call(
        functools.partial(gather_kernel, parts, rows),
        out_shape=jax.ShapeDtypeStruct((16 * rows, width), values.dtype),
        in_specs=[ANY], out_specs=ANY, scratch_shapes=gather_sems(),
        compiler_params=pltpu.CompilerParams(collective_id=collective_id, has_side_effects=True),
        name="gather_stats",
    )(values)


BLOCK_ORDER = (7, 6, 5, 3, 4, 2, 1, 0)


def add_rows(dst, slot_a, src, slot_b, lo, rows, chunk):
    def body(i, carry):
        at = pl.ds(pl.multiple_of(lo + i * chunk, 8), chunk)
        dst[slot_a, at, :] = dst[slot_a, at, :] + src[slot_b, at, :]
        return carry

    lax.fori_loop(0, rows // chunk, body, 0)


def stage_of(color, bits):
    order = ORDERS[color]
    for s in range(3):
        if bits & order[s]:
            return s
    return 3


def box_slot(color, stage, bits):
    rest = subsets(ORDERS[color][stage + 1:])
    return (0, 4, 6)[stage] + rest.index(bits)


def back_kernel(chunks, vocab, inv_n, parts, half, z_ref, emb_ref, st_ref, lab_ref, dz_ref, out_ref,
                acc, pairs, boxes, core_send, core_recv, send_sem, recv_sem, out_sem):
    i = pl.program_id(0)
    me = my_place()

    @pl.when(i == 0)
    def _():
        greet(me, DIMS, True)

    def core_copy(t):
        return pltpu.make_async_remote_copy(
            src_ref=acc.at[8 + t % 2], dst_ref=pairs.at[7 - t], send_sem=core_send.at[t], recv_sem=core_recv.at[t],
            device_id=mesh_id(flipped(me, 0, True)), device_id_type=MESH)

    def chip_copy(color, stage, bits):
        lo, count = parts[color]
        slot = box_slot(color, stage, bits & ~ORDERS[color][stage])
        k = color * 8 + slot
        return pltpu.make_async_remote_copy(
            src_ref=acc.at[bits, pl.ds(lo, count)], dst_ref=boxes.at[slot, pl.ds(lo, count)],
            send_sem=send_sem.at[k], recv_sem=recv_sem.at[k],
            device_id=mesh_id(flipped(me, ORDERS[color][stage])), device_id_type=MESH)

    for t in range(2, 8):
        @pl.when(i == 4 * t)
        def _(t=t):
            core_copy(t - 2).wait_send()

    lab = lab_ref[...]
    top = st_ref[:, 0:1]
    scale = inv_n / st_ref[:, 1:2]
    total = None
    for lo, count in chunks:
        z = z_ref[:, lo:lo + count]
        p = jnp.exp(z - top) * scale
        col = lax.broadcasted_iota(jnp.int32, z.shape, 1)
        p = jnp.where(col == lab - lo, p - inv_n, p)
        if lo + count > vocab:
            p = jnp.where(col < vocab - lo, p, 0.0)
        dz = p.astype(BF)
        dz_ref[:, lo:lo + count] = dz
        part = jnp.dot(dz, emb_ref[lo:lo + count, :], preferred_element_type=F32)
        total = part if total is None else total + part
    t_now = i // 4
    own = (i // 2) % 2
    slot_now = own * (7 - t_now) + (1 - own) * (8 + t_now % 2)
    acc[slot_now, pl.ds(pl.multiple_of((i % 2) * half, half), half), :] = total

    for t in range(8):
        bits = 7 - t

        @pl.when(i == 4 * t + 1)
        def _(t=t):
            core_copy(t).start()

        @pl.when(i == 4 * t + 3)
        def _(t=t, bits=bits):
            core_copy(t).wait_recv()
            for color in range(3):
                lo, count = parts[color]
                add_rows(acc, bits, pairs, bits, lo, count, 16)
                mine = stage_of(color, bits)
                for s in range(mine):
                    chip_copy(color, s, bits | ORDERS[color][s]).wait_recv()
                    add_rows(acc, bits, boxes, box_slot(color, s, bits), lo, count, 16)
                if mine < 3:
                    chip_copy(color, mine, bits).start()

    @pl.when(i == 31)
    def _():
        done = pltpu.make_async_copy(acc.at[0], out_ref, out_sem)
        done.start()
        for t in (6, 7):
            core_copy(t).wait_send()
        for color in range(3):
            for bits in range(1, 8):
                chip_copy(color, stage_of(color, bits), bits).wait_send()
        done.wait()


def head_back(z, emb, stats, labels, parts, vocab, inv_n, collective_id):
    n, padded = z.shape
    d = emb.shape[1]
    rows = n // 16
    half = rows // 2

    def block(i):
        return (device_of(moved(my_place(), 7 - i // 4, 1 - (i // 2) % 2)) * 2 + i % 2, 0)

    return pl.pallas_call(
        functools.partial(back_kernel, make_chunks(padded), vocab, inv_n, parts, half),
        grid=(32,),
        in_specs=[pl.BlockSpec((half, padded), block),
                  pl.BlockSpec((padded, d), lambda i: (0, 0), pipeline_mode=pl.Buffered(1)),
                  pl.BlockSpec((half, 2), block),
                  pl.BlockSpec((half, 1), block)],
        out_specs=[pl.BlockSpec((half, padded), block), ANY],
        out_shape=[jax.ShapeDtypeStruct((n, padded), BF), jax.ShapeDtypeStruct((rows, d), F32)],
        scratch_shapes=[pltpu.VMEM((10, rows, d), F32), pltpu.VMEM((8, rows, d), F32), pltpu.VMEM((7, rows, d), F32),
                        DMA((8,)), DMA((8,)),
                        DMA((24,)), DMA((24,)), DMA],
        compiler_params=pltpu.CompilerParams(collective_id=collective_id, has_side_effects=True, vmem_limit_bytes=VMEM_LIMIT,
                                             ),
        name="head_back",
    )(z, emb, stats, labels)


def tail_kernel(chunks, vocab, views, swap_rows, dz_ref, hn_ref, *refs):
    n_in = max(v[0] for v in views) + 2
    ins, rows_ref = refs[:n_in - 1], refs[n_in - 1]
    de_ref = refs[n_in]
    outs = refs[n_in + 1:n_in + 4]
    back_ref = refs[n_in + 4]
    rest = refs[n_in + 5:]
    accs, pairs, boxes = rest[0:3], rest[3:6], rest[6:9]
    (load_sem, core_send, core_recv, send_sem, recv_sem, out_sem, sp_send, sp_recv, row_send, row_recv, row_sem) = rest[9:]
    i = pl.program_id(0)
    me = my_place()

    def source(color, place):
        which, rows, start, col, cols = views[color]
        m, f = mesh_id(place)
        return ins[which].at[pl.ds(pl.multiple_of(start(m, f), 8), rows), pl.ds(col, cols)]

    def load(color, bits):
        return pltpu.make_async_copy(source(color, flipped(me, bits)), accs[color].at[bits], load_sem.at[color * 8 + bits])

    def core_copy(color, bits):
        k = color * 8 + bits
        return pltpu.make_async_remote_copy(
            src_ref=source(color, flipped(me, bits, True)), dst_ref=pairs[color].at[bits],
            send_sem=core_send.at[k], recv_sem=core_recv.at[k],
            device_id=mesh_id(flipped(me, 0, True)), device_id_type=MESH)

    def chip_copy(color, stage, bits):
        slot = box_slot(color, stage, bits & ~ORDERS[color][stage])
        k = color * 8 + slot
        return pltpu.make_async_remote_copy(
            src_ref=accs[color].at[bits], dst_ref=boxes[color].at[slot],
            send_sem=send_sem.at[k], recv_sem=recv_sem.at[k],
            device_id=mesh_id(flipped(me, ORDERS[color][stage])), device_id_type=MESH)

    def row_copy(bits, core):
        k = 2 * bits + int(core)
        peer = flipped(me, bits, core)
        return pltpu.make_async_remote_copy(
            src_ref=rows_ref.at[pl.ds(pl.multiple_of(device_of(peer) * swap_rows, 8), swap_rows)],
            dst_ref=back_ref.at[pl.ds(pl.multiple_of(device_of(me) * swap_rows, 8), swap_rows)],
            send_sem=row_send.at[k], recv_sem=row_recv.at[k], device_id=mesh_id(peer), device_id_type=MESH)

    def row_arrival(bits, core):
        k = 2 * bits + int(core)
        peer = flipped(me, bits, core)
        dst = back_ref.at[pl.ds(pl.multiple_of(device_of(peer) * swap_rows, 8), swap_rows)]
        return pltpu.make_async_remote_copy(
            src_ref=dst, dst_ref=dst, send_sem=row_send.at[k], recv_sem=row_recv.at[k],
            device_id=mesh_id(peer), device_id_type=MESH)

    own_rows = pl.ds(pl.multiple_of(device_of(me) * swap_rows, 8), swap_rows)
    row_local = pltpu.make_async_copy(rows_ref.at[own_rows], back_ref.at[own_rows], row_sem)
    others = [(b, c) for b in BLOCK_ORDER for c in (False, True) if b or c]

    halves = ((2, 4), (4, 2))

    def target(color, place, half):
        rows = views[color][1]
        m, f = mesh_id(place)
        return outs[color].at[pl.ds(pl.multiple_of(m * rows + half * (rows // 2), 8), rows // 2)]

    def spread_copy(color, half, step, bits):
        rows = views[color][1]
        first, second = halves[half]
        src = accs[color].at[0, pl.ds(half * (rows // 2), rows // 2)] if bits == 0 else target(color, flipped(me, bits), half)
        k = (color * 2 + half) * 3 + step
        return pltpu.make_async_remote_copy(
            src_ref=src, dst_ref=target(color, flipped(me, bits), half),
            send_sem=sp_send.at[k], recv_sem=sp_recv.at[k],
            device_id=mesh_id(flipped(me, first if step == 0 else second)), device_id_type=MESH)

    def out_copy(color):
        rows = views[color][1]
        m, f = mesh_id(me)
        return pltpu.make_async_copy(accs[color].at[0], outs[color].at[pl.ds(pl.multiple_of(m * rows, 8), rows)], out_sem.at[color])

    @pl.when(i == 0)
    def _():
        barrier = pltpu.get_barrier_semaphore()
        for bits, core in others:
            pl.semaphore_signal(barrier, inc=1, device_id=mesh_id(flipped(me, bits, core)), device_id_type=MESH)
        pl.semaphore_wait(barrier, len(others))
        for bits in BLOCK_ORDER:
            for color in range(3):
                core_copy(color, bits).start()
                load(color, bits).start()
        row_local.start()
        de_ref[...] = jnp.zeros_like(de_ref)

    hn = hn_ref[...]
    for lo, count in chunks:
        keep = min(count, vocab - lo)
        part = lax.dot_general(dz_ref[:, lo:lo + count], hn, TN, preferred_element_type=F32)
        de_ref[lo:lo + keep, :] += part[:keep]

    for t in range(8):
        bits = BLOCK_ORDER[t]

        @pl.when(i == t)
        def _(bits=bits):
            for color in range(3):
                rows = views[color][1]
                load(color, bits).wait()
                core_copy(color, bits).wait_recv()
                add_rows(accs[color], bits, pairs[color], bits, 0, rows, 8)
                if stage_of(color, bits) == 0:
                    chip_copy(color, 0, bits).start()

    @pl.when(i == 8)
    def _():
        for bits, core in others:
            row_copy(bits, core).start()

    def arrivals(stage, index):
        for color in range(3):
            order = ORDERS[color]
            bits = sorted(subsets(order[stage + 1:]), key=lambda b: stage_of(color, b))[index]
            slot = box_slot(color, stage, bits)
            chip_copy(color, stage, bits | order[stage]).wait_recv()
            add_rows(accs[color], bits, boxes[color], slot, 0, views[color][1], 8)
            if stage_of(color, bits) == stage + 1 and stage < 2:
                chip_copy(color, stage + 1, bits).start()

    for step, (stage, index) in enumerate([(s, j) for s in range(2) for j in range(4 >> s)]):
        @pl.when(i == 9 + step)
        def _(stage=stage, index=index):
            arrivals(stage, index)

    @pl.when(i == 15)
    def _():
        arrivals(2, 0)
        for color in range(3):
            out_copy(color).start()
            for half in range(2):
                for step in range(2):
                    spread_copy(color, half, step, 0).start()
        for color in range(3):
            for half in range(2):
                spread_copy(color, half, 0, halves[half][0]).wait_recv()
                spread_copy(color, half, 2, halves[half][0]).start()
        for bits, core in others:
            row_arrival(bits, core).wait_recv()
        for color in range(3):
            for half in range(2):
                first, second = halves[half]
                spread_copy(color, half, 1, second).wait_recv()
                spread_copy(color, half, 2, first | second).wait_recv()
        for color in range(3):
            for bits in range(8):
                core_copy(color, bits).wait_send()
                if bits:
                    chip_copy(color, stage_of(color, bits), bits).wait_send()
            for half in range(2):
                for step in range(3):
                    spread_copy(color, half, step, halves[half][0] if step == 2 else 0).wait_send()
            out_copy(color).wait()
        for bits, core in others:
            row_copy(bits, core).wait_send()
        row_local.wait()


def tail_all(dz, hn, arrays, rows, views, piece_shapes, vocab, swap_rows, collective_id):
    n, padded = dz.shape
    d = hn.shape[1]
    block = n // 16
    scratch = []
    for count in (8, 8, 7):
        for shape in piece_shapes:
            scratch.append(pltpu.VMEM((count,) + shape, F32))
    sems = [DMA((24,))] * 5 + [DMA((3,))] + [DMA((18,))] * 2 + [DMA((16,))] * 2 + [DMA]
    return pl.pallas_call(
        functools.partial(tail_kernel, make_chunks(padded), vocab, views, swap_rows),
        grid=(16,),
        in_specs=[pl.BlockSpec((block, padded), lambda i: (i, 0)), pl.BlockSpec((block, d), lambda i: (i, 0))]
        + [ANY] * (len(arrays) + 1),
        out_specs=[pl.BlockSpec((vocab, d), lambda i: (0, 0), pipeline_mode=pl.Buffered(1))] + [ANY] * 4,
        out_shape=[jax.ShapeDtypeStruct((vocab, d), F32)]
        + [jax.ShapeDtypeStruct((4 * r, c), F32) for r, c in piece_shapes]
        + [jax.ShapeDtypeStruct(rows.shape, F32)],
        scratch_shapes=scratch + sems,
        compiler_params=pltpu.CompilerParams(collective_id=collective_id, has_side_effects=True, vmem_limit_bytes=VMEM_LIMIT,
                                             ),
        name="tail_all",
    )(dz, hn, *arrays, rows)


def moved(place, bits, core):
    x, y, z, c = place
    flips = (bits % 2, (bits // 2) % 2, bits // 4, core)
    return tuple(p + q - 2 * p * q for p, q in zip((x, y, z, c), flips))


ARRIVALS = {1: ((0, 0), (1, 0), (2, 0)), 2: ((1, 1),), 3: ((2, 1),), 4: ((2, 2),), 7: ((2, 3),)}


def logits_kernel(chunks, vocab, parts, rows, in_ref, emb_ref, lab_ref, all_ref, z_ref, st_ref, blocks, load_sem, *sems):
    i = pl.program_id(0)
    me = my_place()
    g = Gather(me, parts, rows, in_ref, all_ref, *sems)

    def load(step):
        at = device_of(moved(me, step // 2, step % 2)) * rows
        return pltpu.make_async_copy(all_ref.at[pl.ds(pl.multiple_of(at, CHUNK), rows)], blocks.at[step % 2], load_sem.at[step % 2])

    first = pltpu.make_async_copy(in_ref, blocks.at[0], load_sem.at[0])

    @pl.when(i == 0)
    def _():
        g.begin()
        first.start()

    for step, groups in ARRIVALS.items():
        @pl.when(i == step)
        def _(groups=groups):
            for stage, index in groups:
                g.arrive(stage, index)

    for bits in range(8):
        @pl.when(i == 2 * bits)
        def _(bits=bits):
            g.core_arrive(bits)

    @pl.when(i < 15)
    def _():
        load(i + 1).start()

    load(i).wait()
    hn = blocks[i % 2]
    lab = lab_ref[...]
    top = lab_z = total = None
    for lo, count in chunks:
        z = lax.dot_general(hn, emb_ref[lo:lo + count, :], NT, preferred_element_type=F32)
        z_ref[:, lo:lo + count] = z
        col = lax.broadcasted_iota(jnp.int32, z.shape, 1)
        picked = jnp.sum(jnp.where(col == lab - lo, z, 0.0), axis=1, keepdims=True)
        if lo + count > vocab:
            z = jnp.where(col < vocab - lo, z, -jnp.inf)
        peak = jnp.max(z, axis=1, keepdims=True)
        top = peak if top is None else jnp.maximum(top, peak)
        lab_z = picked if lab_z is None else lab_z + picked
    for lo, count in chunks:
        z = z_ref[:, lo:lo + count]
        e = jnp.exp(z - top)
        if lo + count > vocab:
            col = lax.broadcasted_iota(jnp.int32, z.shape, 1)
            e = jnp.where(col < vocab - lo, e, 0.0)
        part = jnp.sum(e, axis=1, keepdims=True)
        total = part if total is None else total + part
    lane = lax.broadcasted_iota(jnp.int32, (rows, 128), 1)
    packed = jnp.where(lane == 0, top, jnp.where(lane == 1, total, lab_z))
    st_ref[...] = packed.T[:CHUNK]

    @pl.when(i == 15)
    def _():
        g.finish()


def make_chunks(padded):
    units = padded // 128
    count = (units + 7) // 8
    out, lo = [], 0
    for k in range(count, 0, -1):
        take = min(units, ((units + k - 1) // k + 1) // 2 * 2)
        out.append((lo, take * 128))
        lo += take * 128
        units -= take
    return tuple(out)


def head_logits(hn, emb, labels, parts, vocab, collective_id):
    rows, d = hn.shape
    n = 16 * rows
    padded = emb.shape[0]

    def block(i):
        return (device_of(moved(my_place(), i // 2, i % 2)), 0)

    return pl.pallas_call(
        functools.partial(logits_kernel, make_chunks(padded), vocab, parts, rows),
        grid=(16,),
        in_specs=[ANY, pl.BlockSpec((padded, d), lambda i: (0, 0), pipeline_mode=pl.Buffered(1)), pl.BlockSpec((rows, 1), block)],
        out_specs=[ANY, pl.BlockSpec((rows, padded), block), pl.BlockSpec((CHUNK, rows), block)],
        out_shape=[jax.ShapeDtypeStruct((n, d), BF), jax.ShapeDtypeStruct((n, padded), F32),
                   jax.ShapeDtypeStruct((16 * CHUNK, rows), F32)],
        scratch_shapes=[pltpu.VMEM((2, rows, d), BF), DMA((2,))] + gather_sems(),
        compiler_params=pltpu.CompilerParams(collective_id=collective_id, has_side_effects=True, vmem_limit_bytes=VMEM_LIMIT),
        name="head_logits",
    )(hn, emb, labels)


def mlp_forward(x_emb, gain_in, w_in, w_down):
    normed_in, norm_in_back = jax.vjp(lambda values: rms_scale(values, gain_in), x_emb)
    normed_bf = normed_in.astype(BF)
    both = jnp.dot(normed_bf, w_in, preferred_element_type=F32).astype(BF)
    hidden = w_down.shape[0]
    gate_f = both[:, :hidden].astype(F32)
    up_f = both[:, hidden:].astype(F32)
    gate_sig = jax.nn.sigmoid(gate_f)
    silu_gate = gate_f * gate_sig
    act_bf = (silu_gate * up_f).astype(BF)
    mlp_out = jnp.dot(act_bf, w_down, preferred_element_type=F32).astype(BF)
    h_res = x_emb + mlp_out.astype(F32)
    return h_res, (norm_in_back, normed_bf, gate_f, up_f, gate_sig, silu_gate, act_bf)


def mlp_backward(d_hidden, saved, w_in, w_down):
    norm_in_back, normed_bf, gate_f, up_f, gate_sig, silu_gate, act_bf = saved
    d_mlp = d_hidden.astype(BF)
    d_act = jnp.einsum("td,fd->tf", d_mlp, w_down, preferred_element_type=F32)
    grad_down = jnp.einsum("tf,td->fd", act_bf, d_mlp, preferred_element_type=F32)
    d_gate = (d_act * up_f * (gate_sig * (1.0 + gate_f * (1.0 - gate_sig)))).astype(BF)
    d_up = (d_act * silu_gate).astype(BF)
    d_both = jnp.concatenate([d_gate, d_up], axis=1)
    grad_in = jnp.einsum("td,tf->df", normed_bf, d_both, preferred_element_type=F32)
    d_normed = jnp.einsum("tf,df->td", d_both, w_in, preferred_element_type=F32)
    d_x = d_hidden + norm_in_back(d_normed)[0]
    return d_x, grad_in, grad_down


HN_PARTS = ((0, 176), (176, 176), (352, 160))
STAT_PARTS = ((0, 8), (8, 8), (16, 8))


def solution(mesh):
    tok_spec = P("fsdp")
    row_spec = P(AXES)
    weight_spec = P("fsdp")

    def device_step(tok_ids, tok_labels, table_shard, gate_shard, up_shard, down_shard, gain_in, gain_out):
        m_idx = lax.axis_index("model")
        f_idx = lax.axis_index("fsdp")
        me = m_idx * 4 + f_idx
        vocab, width = table_shard.shape
        own = tok_ids.shape[0] * tok_ids.shape[1] // 4
        num_tokens = own * 16

        def full_weight(shard):
            rows = shard.shape[0] // 4
            piece = lax.dynamic_slice_in_dim(shard, m_idx * rows, rows, axis=0)
            return lax.all_gather(piece, ("fsdp", "model"), axis=0, tiled=True)

        w_in = full_weight(jnp.concatenate([gate_shard, up_shard], axis=1))
        w_down = full_weight(down_shard)
        tokens = lax.all_gather(jnp.stack([tok_ids.reshape(-1), tok_labels.reshape(-1)]), "fsdp", axis=0)
        tokens = tokens.reshape(4, 2, 4, own).transpose(1, 2, 0, 3).reshape(2, 16, own)
        ids, labels = tokens[0], tokens[1].reshape(num_tokens)
        my_ids = lax.dynamic_slice_in_dim(ids, me, 1, axis=0)[0]

        base = vocab * 16
        place = lax.broadcasted_iota(jnp.int32, ids.shape, 1)
        mine = (ids // vocab) == me
        owner = my_ids // vocab
        owner_hot = owner[None, :] == jnp.arange(16, dtype=jnp.int32)[:, None]
        keys = jnp.concatenate([
            jnp.where(mine, place, place + own) * base + ids,
            jnp.where(owner_hot, place, place + own) * base], axis=0)
        keys = lax.sort(keys, dimension=1)
        keys = jnp.pad(keys, ((0, 0), (0, ROUND_ROWS)), constant_values=own * base)
        rank = jnp.sum(jnp.where(owner_hot, jnp.cumsum(owner_hot.astype(jnp.int32), axis=1), 0), axis=0) - 1
        hot_all = (ids // vocab)[:, None, :] == jnp.arange(16, dtype=jnp.int32)[None, :, None]
        most = jnp.max(jnp.sum(hot_all.astype(jnp.int32), axis=2))
        rounds = (most + ROUND_ROWS - 1) // ROUND_ROWS

        def round_keys(first, r):
            key = lax.dynamic_slice(keys, (first, r * ROUND_ROWS), (16, ROUND_ROWS)).reshape(-1)
            return key < own * base, key

        def served(r):
            valid, key = round_keys(0, r)
            return valid, jnp.where(valid, key % base - me * vocab, 0)

        def returned(r):
            valid, key = round_keys(16, r)
            return jnp.where(valid, key // base, 0)

        def take_rows(values, rows):
            return jnp.take(values, rows, axis=0)

        def exchange(values):
            return lax.all_to_all(values, AXES, 0, 0, tiled=True)

        def lookup_round(state):
            r, x = state
            _, row = served(r)
            got = exchange(take_rows(table_shard, row))
            at = rank - r * ROUND_ROWS
            now = (at >= 0) & (at < ROUND_ROWS)
            fetched = take_rows(got, jnp.where(now, owner * ROUND_ROWS + at, 0))
            return r + 1, jnp.where(now[:, None], fetched, x)

        _, x_rows = lax.while_loop(lambda s: s[0] < rounds, lookup_round, lookup_round((jnp.int32(0), jnp.zeros((own, width), BF))))
        x_emb = x_rows.astype(F32)

        h_res, saved = mlp_forward(x_emb, gain_in, w_in, w_down)
        hn_f, norm_out_back = jax.vjp(lambda values: rms_scale(values, gain_out), h_res)
        padded = (vocab + 127) // 128 * 128
        emb = jnp.pad(table_shard, ((0, padded - vocab), (0, 0)))
        loc_labels = labels - me * vocab
        in_here = (loc_labels >= 0) & (loc_labels < vocab)
        lab_col = jnp.where(in_here, loc_labels, -1).reshape(num_tokens, 1)
        hn_bf, z, local_stats = head_logits(hn_f.astype(BF), emb, lab_col, HN_PARTS, vocab, 0)
        packed = local_stats.reshape(16, CHUNK, own)[:, :3].transpose(1, 0, 2).reshape(24, num_tokens // 8)
        all_stats = gather_all(packed, STAT_PARTS, 1).reshape(16, 3, num_tokens)
        tops = all_stats[:, 0]
        row_max = jnp.max(tops, axis=0)
        sum_exp = jnp.sum(all_stats[:, 1] * jnp.exp(tops - row_max[None, :]), axis=0)
        label_logit = jnp.sum(all_stats[:, 2], axis=0)
        loss = jnp.sum(row_max + jnp.log(sum_exp) - label_logit) / num_tokens
        stat_cols = jnp.stack([row_max, sum_exp], axis=1)
        dz, d_hn = head_back(z, emb, stat_cols, lab_col, HN_PARTS, vocab, 1.0 / num_tokens, 2)
        d_hidden = norm_out_back(d_hn)[0]
        d_x, g_in, g_down = mlp_backward(d_hidden, saved, w_in, w_down)

        g_rows, hidden = w_in.shape[0] // 16, w_down.shape[0]
        d_rows = hidden // 16
        views = (
            (0, g_rows, lambda m, f: f * (4 * g_rows) + m * g_rows, 0, hidden),
            (0, g_rows, lambda m, f: f * (4 * g_rows) + m * g_rows, hidden, hidden),
            (1, d_rows, lambda m, f: f * (4 * d_rows) + m * d_rows, 0, width),
        )
        pieces = [(g_rows, hidden), (g_rows, hidden), (d_rows, width)]
        sent = take_rows(d_x, returned(0))
        d_head, grad_gate, grad_up, grad_down, got = tail_all(
            dz, hn_bf, [g_in, g_down], sent, views, pieces, vocab, ROUND_ROWS, 3)

        def add_round(grad, r, got):
            valid, row = served(r)
            return grad.at[row].add(jnp.where(valid[:, None], got, 0.0))

        def grad_round(state):
            r, grad = state
            return r + 1, add_round(grad, r, exchange(take_rows(d_x, returned(r))))

        _, grad_table = lax.while_loop(lambda s: s[0] < rounds, grad_round, (jnp.int32(1), add_round(d_head, 0, got)))
        return loss, grad_table, grad_gate, grad_up, grad_down

    return jax.shard_map(device_step, mesh=mesh, in_specs=(tok_spec, tok_spec, row_spec, weight_spec, weight_spec, weight_spec, P(), P()), out_specs=(P(), row_spec, weight_spec, weight_spec, weight_spec), check_vma=False)
```
